256 devices in a mesh: rep: 2 (over y_hi), fsdp: 128 (over z, x, y_lo, core).
Axes of the slice: x: 4, y: 4 (y_hi: 2, y_lo: 2; y = y_hi * 2 + y_lo), z: 8, core: 2. Of those that a mesh axis runs over, the one named last changes fastest.
Arguments:
- tokens: bfloat16 [131072, 4096], P(('rep', 'fsdp')), may hold values from -24 to 24
- value_cot: bfloat16 [131072, 1024], P(('rep', 'fsdp')), may hold values from -6 to 6
- value_weight: bfloat16 [2, 4096, 1024], P('rep', 'fsdp'), may hold values from -0.09375 to 0.09375
- global_params: float32 [16777216], P('fsdp'), may hold values from -6 to 6
- local_params: float32 [2, 16777216], P('rep', 'fsdp'), may hold values from -6 to 6
- momentum: float32 [16777216], P('fsdp'), may hold values from -3 to 3
Outputs:
- token_grad: bfloat16 [131072, 4096], P(('rep', 'fsdp'))
- value_grad: float32 [2, 4096, 1024], P('rep', 'fsdp')
- new_global: float32 [16777216], P('fsdp')
- new_moment: float32 [16777216], P('fsdp')
The draws below stay inside these ranges and needn't reach their ends.
All inputs are finite; a program needn't handle non-finite values.
Results may differ from the reference program's by a relative error of at most 0.001.
Values may be sent and summed in bfloat16 or wider, within the bound.
No kernel may reach another device: no remote copies, remote signals or barrier semaphores. Data moves between devices by JAX's collectives and lax.ppermute only.
A program may use at most 128 MiB of HBM per device.

```python
import jax
import jax.numpy as jnp
from jax import lax

D = 4096
KVW = 1024
REPS = 2
GROUP_TOK = 65536
TOKENS = 131072
FRAG = 16777216
N_REP = 2


def spiked(drawn, rng, source, target, shards_of, factor):
    def block_of(dim):
        return (jnp.arange(drawn.shape[dim]) // (drawn.shape[dim] // shards_of)).reshape((-1,) + (1,) * (drawn.ndim - 1 - dim))

    first = jax.random.permutation(rng, shards_of)[block_of(target)]
    far = (block_of(target) + shards_of // 2) % shards_of
    return jnp.where((block_of(source) == first) | (block_of(source) == far), factor * drawn, drawn)


def block_levels(stream_key, extent, shards, smallest, top_value):
    def one(dim, shards_of):
        draws = jax.random.uniform(jax.random.fold_in(jax.random.fold_in(stream_key, 6), dim), (shards_of,), jnp.float32, smallest / len(shards), top_value / len(shards))
        return jnp.repeat(jnp.exp(draws), extent[dim] // shards_of).reshape((-1,) + (1,) * (len(extent) - dim - 1))

    level = one(*shards[0])
    for cut in shards[1:]:
        level = level * one(*cut)
    return level


def noise(key, dims, spread, reach, pieces=(), held_as=jnp.bfloat16):
    drawn = spread * jax.random.normal(key, dims, jnp.float32)
    if pieces:
        drawn = drawn * block_levels(key, dims, pieces, -0.22, 0.18)
    return jnp.clip(drawn, -reach, reach).astype(held_as)


def heavy_noise(stream_key, dims, scale, reach, pieces, heavy, dtype=jnp.bfloat16):
    array = scale * jax.random.normal(stream_key, dims, jnp.float32)
    if pieces:
        array = array * block_levels(stream_key, dims, pieces, -0.22, 0.18)
    return jnp.clip(spiked(array, jax.random.fold_in(stream_key, 3), *heavy), -reach, reach).astype(dtype)


def setup_inputs(seed: int = 0) -> dict:
    keys = jax.random.split(jax.random.key(seed), 7)
    return {
        "tokens": heavy_noise(keys[0], (TOKENS, D), 1.0, 24.0, ((0, 256),), (0, 1, 256, 6.0)),
        "value_cot": noise(keys[1], (TOKENS, KVW), 1.0, 6.0, ((0, 256),)),
        "value_weight": noise(keys[2], (REPS, D, KVW), D ** -0.5, 0.09375, ((0, 2), (1, 128))),
        "global_params": noise(keys[3], (FRAG,), 1.0, 6.0, ((0, 128),), jnp.float32),
        "local_params": noise(keys[4], (REPS, FRAG), 1.0, 6.0, ((0, 2), (1, 128)), jnp.float32),
        "momentum": noise(keys[5], (FRAG,), 0.5, 3.0, ((0, 128),), jnp.float32),
    }


def reference(tokens, value_cot, value_weight, global_params, local_params, momentum):
    token_parts = []
    grad_parts = []
    for replica in range(N_REP):
        inputs = tokens[replica * GROUP_TOK:(replica + 1) * GROUP_TOK]
        cotan = value_cot[replica * GROUP_TOK:(replica + 1) * GROUP_TOK]
        token_parts.append(jnp.dot(cotan, value_weight[replica].T, preferred_element_type=jnp.float32).astype(jnp.bfloat16))
        summed = jnp.dot(inputs.T, cotan, preferred_element_type=jnp.float32)
        grad_parts.append(summed * (1.0 / jnp.sqrt(jnp.float32(GROUP_TOK))))
    token_grad = jnp.concatenate(token_parts, axis=0)
    value_grad = jnp.stack(grad_parts, axis=0)
    pseudo = global_params - lax.optimization_barrier(jnp.sum(local_params, axis=0)) / N_REP
    new_moment = 0.9 * momentum + pseudo
    new_global = global_params - 0.7 * (pseudo + 0.9 * new_moment)
    return (token_grad, value_grad, new_global, new_moment)
```

```python
import functools

import jax
import jax.numpy as jnp
from jax import lax
from jax.experimental import pallas as pl
from jax.experimental.pallas import tpu as pltpu
from jax.sharding import Mesh
from jax.sharding import PartitionSpec as P


FSDP = ("z", "x", "y", "c")
REP_FSDP = ("rep", "z", "x", "y", "c")
NZ, NX = 8, 4
SWAP = [(0, 1), (1, 0)]
Z_STEP = [(2 * i + c, 2 * ((i + 1 - 2 * c) % NZ) + c) for i in range(NZ) for c in range(2)]
Z_UP = [(2 * i, 2 * ((i + 1) % NZ)) for i in range(NZ)]
X_STEP = [(2 * i + c, 2 * ((i + 1 - 2 * c) % NX) + c) for i in range(NX) for c in range(2)]
X_FAR = [(i, (i + 2) % NX) for i in range(NX)]
TOP = 14.0
TAIL = 16
F32 = jnp.float32


def pack(value, bound):
    body = (value * jnp.exp2(TOP - bound)).astype(jnp.float16)
    tail = jnp.broadcast_to(bound.astype(jnp.float16), (TAIL, value.shape[1]))
    return jnp.concatenate([body, tail], axis=0)


def unpack(message):
    bound = message[-1, 0].astype(F32)
    return message[:-TAIL].astype(F32) * jnp.exp2(bound - TOP), bound


def term_kernel(_, *refs):
    *cols, cot_a, cot_b, out, bound = refs
    dims = (((0,), (0,)), ((), ()))
    mine = jnp.concatenate([r[...] for r in cols[:4]], axis=1)
    total = lax.dot_general(mine, cot_a[...], dims, preferred_element_type=F32)
    theirs = jnp.concatenate([r[...] for r in cols[4:]], axis=1)
    total += lax.dot_general(theirs, cot_b[...], dims, preferred_element_type=F32)
    out[...] = total
    top = jnp.maximum(jnp.max(jnp.abs(total)), 1e-30)
    bound[...] = jnp.ceil(jnp.log2(jnp.full(bound.shape, top, F32))) + 1.0


def grad_term(chunks, tokens, cot, other_tokens, other_cot):
    rows, width = cot.shape
    spec = [pl.BlockSpec((rows, 128), functools.partial(lambda k, i, ids: (0, ids[k]), k)) for k in range(4)]
    whole = pl.BlockSpec((rows, width), lambda i, ids: (0, 0))
    term, bound = pl.pallas_call(
        term_kernel,
        grid_spec=pltpu.PrefetchScalarGridSpec(
            num_scalar_prefetch=1,
            grid=(1,),
            in_specs=spec + spec + [whole, whole],
            out_specs=[
                pl.BlockSpec((512, width), lambda i, ids: (0, 0)),
                pl.BlockSpec((8, 128), lambda i, ids: (0, 0)),
            ],
        ),
        out_shape=[jax.ShapeDtypeStruct((512, width), F32), jax.ShapeDtypeStruct((8, 128), F32)],
        cost_estimate=pl.CostEstimate(flops=4 * rows * 512 * width, bytes_accessed=6 << 20, transcendentals=0),
    )(chunks, *[tokens] * 4, *[other_tokens] * 4, cot, other_cot)
    return term, bound[0, 0]


def sum_grad(tokens, cot, factor):
    z, x, y, c = (lax.axis_index(a) for a in FSDP)
    sign = 1 - 2 * c
    other_cot = lax.ppermute(cot, "c", SWAP)
    other_tokens = lax.ppermute(tokens, "c", SWAP)
    steps = jnp.arange(4)
    up = (z + 4 - steps) % NZ
    down = jnp.where(steps == 0, z, z + 4 + steps) % NZ
    mine, theirs = jnp.where(c == 0, up, down), jnp.where(c == 0, down, up)
    near, far = (x + sign) % NX, (x + 2) % NX
    term = lambda rows, col: grad_term((rows * NX + col).astype(jnp.int32), tokens, cot, other_tokens, other_cot)
    far_term, e = term(mine, far)
    from_far = lax.ppermute(pack(far_term, e), ("x", "c"), X_STEP)
    near_term, e = term(theirs, near)
    cross = lax.ppermute(pack(near_term, e), ("x", "c"), X_STEP)
    cross = lax.ppermute(cross, "c", SWAP)
    near_term, e = term(mine, near)
    came, came_e = unpack(from_far)
    direct = lax.ppermute(pack(near_term + came, jnp.maximum(e, came_e) + 1), ("x", "c"), X_STEP)
    total, e = term(mine, x)
    a, ae = unpack(cross)
    b, be = unpack(direct)
    total = (total + a + b).reshape(4, 128, -1)
    e = jnp.maximum(jnp.maximum(e, ae), be) + 2
    message = lax.ppermute(pack(total[0], e), ("z", "c"), Z_UP)
    for k in range(1, 4):
        came, came_e = unpack(message)
        if k == 1:
            came = jnp.where(c == 0, came, 0.0)
            came_e = jnp.where(c == 0, came_e, e)
        message = lax.ppermute(pack(total[k] + came, jnp.maximum(e, came_e) + 1), ("z", "c"), Z_STEP)
    came, _ = unpack(message)
    came = (came + jnp.where(c == 0, 0.0, total[0])).reshape(2, 2, 32, -1)
    pick = lambda v, i, dim: lax.dynamic_index_in_dim(v, i, dim, keepdims=False)
    rows = pick(came, c, 1) + lax.ppermute(pick(came, 1 - c, 1), "c", SWAP)
    return (pick(rows, y, 0) + lax.ppermute(pick(rows, 1 - y, 0), "y", SWAP)) * factor


def token_kernel(where, *refs, count, halves):
    cot, blocks, out = refs[0], refs[1 : 1 + count], refs[-1]
    x = where[2]

    def one(block, base):
        got = lax.dot_general(
            cot[...], block[...], (((1,), (1,)), ((), ())), preferred_element_type=F32
        ).astype(out.dtype)
        for k in range(block.shape[0] // 128):
            col = lax.rem(x + base + k, NX)
            out[:, pl.ds(pl.multiple_of(col * 128, 128), 128)] = got[:, k * 128 : (k + 1) * 128]

    if halves:
        for k in range(count):
            one(blocks[k], where[3 + k])
    else:
        for k in range(count):
            pl.when(pl.program_id(0) == k)(functools.partial(one, blocks[k], 0))


def token_part(where, cot, blocks, done, halves=False):
    rows, width = cot.shape
    count = len(blocks)
    full = lambda s: pl.BlockSpec(s, lambda i, w: (0, 0))
    extra = [] if done is None else [done]
    size = sum(b.shape[0] for b in blocks)
    return pl.pallas_call(
        functools.partial(token_kernel, count=count, halves=halves),
        grid_spec=pltpu.PrefetchScalarGridSpec(
            num_scalar_prefetch=1,
            grid=(1 if halves else count,),
            in_specs=[full((rows, width))]
            + [full(b.shape) for b in blocks]
            + [pl.BlockSpec(memory_space=pl.ANY)] * len(extra),
            out_specs=pl.BlockSpec((rows, 512), lambda i, w: (0, w[i])),
        ),
        out_shape=jax.ShapeDtypeStruct((rows, 4096), jnp.bfloat16),
        input_output_aliases={2 + count: 0} if extra else {},
        cost_estimate=pl.CostEstimate(flops=2 * rows * size * width, bytes_accessed=4 << 20, transcendentals=0),
    )(where, cot, *blocks, *extra)


def token_grads(cot, weight):
    z, x, y, c = (lax.axis_index(a) for a in FSDP)
    sign = 1 - 2 * c
    order = lambda first, mine, other: jnp.where(first, jnp.concatenate([mine, other], 0), jnp.concatenate([other, mine], 0))
    pair = order(y == 0, weight[None], lax.ppermute(weight, "y", SWAP)[None])
    other = lax.ppermute(pair, "c", SWAP)
    block = order(c == 0, pair[:, None].swapaxes(0, 1), other[:, None].swapaxes(0, 1)).swapaxes(0, 1)
    block = block.reshape(128, -1)
    side = lax.ppermute(block, ("x", "c"), X_STEP)
    far = lax.ppermute(lax.dynamic_slice_in_dim(block, 64 * c, 64, 0), "x", X_FAR)
    across = lax.ppermute(jnp.concatenate([side, far], 0), "c", SWAP)
    up = jnp.where(c == 0, across[:128], side)
    down = jnp.where(c == 0, side, across[:128])
    far = order(c == 0, far, across[128:])
    block = jnp.concatenate([block, up, far, down], 0)
    scalars = lambda *v: jnp.stack([jnp.asarray(s, jnp.int32) for s in v])
    grad = token_part(scalars(z, 0, x, 0, 0), cot, [block], None)
    for k in range(1, 4):
        block = lax.ppermute(block, ("z", "c"), Z_STEP)
        other = lax.ppermute(block, "c", SWAP)
        grad = token_part(scalars((z - k * sign) % NZ, (z + k * sign) % NZ, x, 0, 0), cot, [block, other], grad)
    block = lax.ppermute(lax.dynamic_slice_in_dim(block, 256 * c, 256, 0), ("z", "c"), Z_STEP)
    other = lax.ppermute(block, "c", SWAP)
    return token_part(scalars((z + 4) % NZ, 0, x, 2 * c, 2 - 2 * c), cot, [block, other], grad, halves=True)


def shards(tokens, value_cot, value_weight, global_params, local_params, momentum):
    mine = local_params[0]
    totals = mine + lax.ppermute(mine, "rep", SWAP)
    factor = 1.0 / jnp.sqrt(jnp.float32(tokens.shape[0] * lax.axis_size(FSDP)))
    token_grad = token_grads(value_cot, value_weight[0])
    value_grad = sum_grad(tokens, value_cot, factor)[None]
    pseudo = global_params - totals / lax.axis_size("rep")
    new_moment = 0.9 * momentum + pseudo
    new_global = global_params - 0.7 * (pseudo + 0.9 * new_moment)
    return (token_grad, value_grad, new_global, new_moment)


def solution(mesh):
    split = Mesh(mesh.devices.reshape(mesh.shape["rep"], NZ, NX, 2, 2), REP_FSDP)
    return jax.shard_map(
        shards,
        mesh=split,
        in_specs=(
            P(REP_FSDP, None),
            P(REP_FSDP, None),
            P("rep", FSDP, None),
            P(FSDP),
            P("rep", FSDP),
            P(FSDP),
        ),
        out_specs=(P(REP_FSDP, None), P("rep", FSDP, None), P(FSDP), P(FSDP)),
        check_vma=False,
    )
```

```python
import functools

import jax
import jax.numpy as jnp
from jax import lax
from jax.experimental import pallas as pl
from jax.experimental.pallas import tpu as pltpu
from jax.sharding import Mesh
from jax.sharding import PartitionSpec as P


FSDP = ("z", "x", "y", "c")
REP_FSDP = ("rep", "z", "x", "y", "c")
NZ, NX = 8, 4
SWAP = [(0, 1), (1, 0)]
Z_STEP = [(2 * i + c, 2 * ((i + 1 - 2 * c) % NZ) + c) for i in range(NZ) for c in range(2)]
Z_UP = [(2 * i, 2 * ((i + 1) % NZ)) for i in range(NZ)]
X_STEP = [(2 * i + c, 2 * ((i + 1 - 2 * c) % NX) + c) for i in range(NX) for c in range(2)]
F32 = jnp.float32
DATA, TAIL = 128, 8
BLOCK = DATA + TAIL


def tall(value):
    return value.reshape(-1, BLOCK, value.shape[-1])


def with_tails(body, up):
    row = lax.broadcasted_iota(jnp.int32, body.shape, 1)
    return jnp.where(row < DATA, body, up)


def scale_row(value):
    return value[0:1, DATA : DATA + 1].astype(F32)


def fourth(v):
    return (v * v) * (v * v)


def combine(*parts):
    ups = [scale_row(p) for p in parts]
    up = functools.reduce(jnp.maximum, ups)
    inverse = 1.0 / up
    body = sum(p.astype(F32) * fourth(u * inverse) for p, u in zip(parts, ups))
    return with_tails(body, up)


def term_kernel(_, *refs):
    *cols, cot_a, cot_b, out = refs
    dims = (((0,), (0,)), ((), ()))
    mine = jnp.concatenate([r[...] for r in cols[:4]], axis=1)
    total = lax.dot_general(mine, cot_a[...], dims, preferred_element_type=F32)
    theirs = jnp.concatenate([r[...] for r in cols[4:]], axis=1)
    total += lax.dot_general(theirs, cot_b[...], dims, preferred_element_type=F32)
    top = jnp.full((TAIL, out.shape[-1]), jnp.maximum(jnp.max(jnp.abs(total)), 1e-30), F32)
    power = jnp.clip(jnp.ceil((jnp.log2(top) - 8.5) * 0.25), -14.0, 14.0)
    down = fourth(jnp.exp2(-power[:1]))
    up = jnp.exp2(power)
    for k in range(4):
        out[k * BLOCK : k * BLOCK + DATA, :] = total[k * DATA : (k + 1) * DATA] * down
        out[k * BLOCK + DATA : (k + 1) * BLOCK, :] = up


def grad_terms(chunks, tokens, cot, other_tokens, other_cot):
    rows, width = cot.shape
    count = len(chunks)
    ids = jnp.concatenate(chunks).astype(jnp.int32)
    spec = [pl.BlockSpec((rows, DATA), functools.partial(lambda k, i, ids: (0, ids[4 * i + k]), k)) for k in range(4)]
    whole = pl.BlockSpec((rows, width), lambda i, ids: (0, 0))
    call = pl.pallas_call(
        term_kernel,
        grid_spec=pltpu.PrefetchScalarGridSpec(
            num_scalar_prefetch=1,
            grid=(count,),
            in_specs=spec + spec + [whole, whole],
            out_specs=pl.BlockSpec((4 * BLOCK, width), lambda i, ids: (i, 0)),
        ),
        out_shape=jax.ShapeDtypeStruct((4 * BLOCK * count, width), F32),
        cost_estimate=pl.CostEstimate(
            flops=4 * rows * 512 * width * count, bytes_accessed=(2 + 3 * count) << 20, transcendentals=0
        ),
    )
    terms = call(ids, *[tokens] * 4, *[other_tokens] * 4, cot, other_cot)
    return [tall(terms[4 * BLOCK * k : 4 * BLOCK * (k + 1)]) for k in range(count)]


def sum_grad(tokens, cot, factor):
    z, x, y, c = (lax.axis_index(a) for a in FSDP)
    sign = 1 - 2 * c
    other_cot = lax.ppermute(cot, "c", SWAP)
    other_tokens = lax.ppermute(tokens, "c", SWAP)
    half = lambda v: v.astype(jnp.float16)
    steps = jnp.arange(4)
    up = (z + 4 - steps) % NZ
    down = jnp.where(steps == 0, z, z + 4 + steps) % NZ
    mine, theirs = jnp.where(c == 0, up, down), jnp.where(c == 0, down, up)
    near, far = (x + sign) % NX, (x + 2) % NX
    inputs = (tokens, cot, other_tokens, other_cot)
    (far_term,) = grad_terms([mine * NX + far], *inputs)
    from_far = lax.ppermute(half(far_term), ("x", "c"), X_STEP)
    cross, near_term, own_term = grad_terms([theirs * NX + near, mine * NX + near, mine * NX + x], *inputs)
    cross = half(cross)
    from_far, _ = lax.optimization_barrier((from_far, cross))
    cross = lax.ppermute(cross, ("x", "c"), X_STEP)
    cross = lax.ppermute(cross, "c", SWAP)
    direct = lax.ppermute(half(combine(near_term, from_far)), ("x", "c"), X_STEP)
    total = combine(own_term, cross, direct)
    came = lax.ppermute(half(total[0:1]), ("z", "c"), Z_UP)
    for k in range(1, 4):
        came = lax.ppermute(half(combine(total[k : k + 1], came)), ("z", "c"), Z_STEP)
    plain = lambda v: v[0, :DATA].astype(F32) * fourth(scale_row(v)[0])
    came = (plain(came) + jnp.where(c == 0, 0.0, plain(total[0:1]))).reshape(2, 2, 32, -1)
    pick = lambda v, i, dim: lax.dynamic_index_in_dim(v, i, dim, keepdims=False)
    rows = pick(came, c, 1) + lax.ppermute(pick(came, 1 - c, 1), "c", SWAP)
    return (pick(rows, y, 0) + lax.ppermute(pick(rows, 1 - y, 0), "y", SWAP)) * factor


def token_kernel(where, *refs, count, halves):
    cot, blocks, out = refs[0], refs[1 : 1 + count], refs[-1]
    x = where[4]

    def one(block, base):
        got = lax.dot_general(
            cot[...], block[...], (((1,), (1,)), ((), ())), preferred_element_type=F32
        ).astype(out.dtype)
        for k in range(block.shape[0] // 128):
            col = lax.rem(x + base + k, NX)
            out[:, pl.ds(pl.multiple_of(col * 128, 128), 128)] = got[:, k * 128 : (k + 1) * 128]

    if halves:
        for k in range(count):
            one(blocks[k], where[5 + k])
    else:
        for k in range(count):
            pl.when(pl.program_id(0) == k)(functools.partial(one, blocks[k], 0))


def token_part(where, cot, blocks, done, halves=False):
    rows, width = cot.shape
    count = len(blocks)
    full = lambda s: pl.BlockSpec(s, lambda i, w: (0, 0))
    extra = [] if done is None else [done]
    size = sum(b.shape[0] for b in blocks)
    where = jnp.stack([jnp.asarray(v, jnp.int32) for v in where])
    return pl.pallas_call(
        functools.partial(token_kernel, count=count, halves=halves),
        grid_spec=pltpu.PrefetchScalarGridSpec(
            num_scalar_prefetch=1,
            grid=(1 if halves else count,),
            in_specs=[full((rows, width))]
            + [full(b.shape) for b in blocks]
            + [pl.BlockSpec(memory_space=pl.ANY)] * len(extra),
            out_specs=pl.BlockSpec((rows, 512), lambda i, w: (0, w[i])),
        ),
        out_shape=jax.ShapeDtypeStruct((rows, 4096), jnp.bfloat16),
        input_output_aliases={2 + count: 0} if extra else {},
        cost_estimate=pl.CostEstimate(flops=2 * rows * size * width, bytes_accessed=4 << 20, transcendentals=0),
    )(where, cot, *blocks, *extra)


def token_grads(cot, weight):
    z, x, y, c = (lax.axis_index(a) for a in FSDP)
    sign = 1 - 2 * c
    ring = lambda step: [(i, (i + step) % NX) for i in range(NX)]
    other = lax.ppermute(weight, "y", SWAP)
    pair = jnp.where(y == 0, jnp.stack([weight, other]), jnp.stack([other, weight]))
    others = [lax.ppermute(pair, "x", ring(NX - k)) for k in (1, 2, 3)]
    mine = jnp.stack([pair, *others])
    theirs = lax.ppermute(mine, "c", SWAP)
    block = jnp.where(c == 0, jnp.stack([mine, theirs], 2), jnp.stack([theirs, mine], 2)).reshape(512, -1)
    near, swapped = [], []
    own = block
    for _ in range(1, 4):
        block = lax.ppermute(block, ("z", "c"), Z_STEP)
        near.append(block)
        swapped.append(lax.ppermute(block, "c", SWAP))
    block = lax.ppermute(lax.dynamic_slice_in_dim(block, 256 * c, 256, 0), ("z", "c"), Z_STEP)
    other = lax.ppermute(block, "c", SWAP)
    at = lambda k: (z + k * sign) % NZ
    grad = token_part((z, at(-1), at(1), 0, x), cot, [own, near[0], swapped[0]], None)
    grad = token_part((at(-2), at(2), at(-3), at(3), x), cot, [near[1], swapped[1], near[2], swapped[2]], grad)
    return token_part((at(4), 0, 0, 0, x, 2 * c, 2 - 2 * c), cot, [block, other], grad, halves=True)


def step(tokens, value_cot, value_weight, global_params, local_params, momentum):
    mine = local_params[0]
    totals = mine + lax.ppermute(mine, "rep", SWAP)
    factor = 1.0 / jnp.sqrt(jnp.float32(tokens.shape[0] * lax.axis_size(FSDP)))
    token_grad = token_grads(value_cot, value_weight[0])
    value_grad = sum_grad(tokens, value_cot, factor)[None]
    pseudo = global_params - totals / lax.axis_size("rep")
    new_moment = 0.9 * momentum + pseudo
    new_global = global_params - 0.7 * (pseudo + 0.9 * new_moment)
    return (token_grad, value_grad, new_global, new_moment)


def solution(mesh):
    split = Mesh(mesh.devices.reshape(mesh.shape["rep"], NZ, NX, 2, 2), REP_FSDP)
    return jax.shard_map(
        step,
        mesh=split,
        in_specs=(
            P(REP_FSDP, None),
            P(REP_FSDP, None),
            P("rep", FSDP, None),
            P(FSDP),
            P("rep", FSDP),
            P(FSDP),
        ),
        out_specs=(P(REP_FSDP, None), P("rep", FSDP, None), P(FSDP), P(FSDP)),
        check_vma=False,
    )
```

```python
import functools

import jax
import jax.numpy as jnp
from jax import lax
from jax.experimental import pallas as pl
from jax.experimental.pallas import tpu as pltpu
from jax.sharding import Mesh
from jax.sharding import PartitionSpec as P


FSDP = ("z", "x", "y", "c")
REP_FSDP = ("rep", "z", "x", "y", "c")
NZ, NX = 8, 4
SWAP = [(0, 1), (1, 0)]
Z_STEP = [(2 * i + c, 2 * ((i + 1 - 2 * c) % NZ) + c) for i in range(NZ) for c in range(2)]
Z_FAR = [(2 * i, 2 * ((i + 4) % NZ)) for i in range(NZ)]
X_STEP = [(2 * i + c, 2 * ((i + 1 - 2 * c) % NX) + c) for i in range(NX) for c in range(2)]
F32 = jnp.float32
DATA, TAIL = 128, 8
BLOCK = DATA + TAIL


def tall(value):
    return value.reshape(-1, BLOCK, value.shape[-1])


def with_tails(body, up, down):
    row = lax.broadcasted_iota(jnp.int32, body.shape, 1)
    return jnp.where(row < DATA, body, jnp.where(row < DATA + TAIL // 2, up, down))


def scale_rows(value):
    low = DATA + TAIL // 2
    return value[0:1, DATA : DATA + 1].astype(F32), value[0:1, low : low + 1].astype(F32)


def fourth(v):
    return (v * v) * (v * v)


def combine(*parts):
    ups, downs = zip(*[scale_rows(p) for p in parts])
    up = functools.reduce(jnp.maximum, ups)
    down = functools.reduce(jnp.minimum, downs)
    body = sum(p.astype(F32) * fourth(u * down) for p, u in zip(parts, ups))
    return with_tails(body, up, down)


def pick_kernel(_, *refs):
    refs[-1][0] = jnp.concatenate([r[...] for r in refs[:4]], axis=1)


def column_specs(rows):
    return [pl.BlockSpec((rows, DATA), functools.partial(lambda k, i, ids: (0, ids[4 * i + k]), k)) for k in range(4)]


def pick_columns(chunks, tokens):
    rows = tokens.shape[0]
    count = len(chunks)
    return pl.pallas_call(
        pick_kernel,
        grid_spec=pltpu.PrefetchScalarGridSpec(
            num_scalar_prefetch=1,
            grid=(count,),
            in_specs=column_specs(rows),
            out_specs=pl.BlockSpec((1, rows, 512), lambda i, ids: (i, 0, 0)),
        ),
        out_shape=jax.ShapeDtypeStruct((count, rows, 512), tokens.dtype),
        compiler_params=pltpu.CompilerParams(vmem_limit_bytes=16 << 20),
        cost_estimate=pl.CostEstimate(flops=rows * 512 * count, bytes_accessed=count << 20, transcendentals=0),
    )(jnp.concatenate(chunks).astype(jnp.int32), *[tokens] * 4)


def term_kernel(_, *refs):
    *cols, theirs, cot_a, cot_b, out = refs
    dims = (((0,), (0,)), ((), ()))
    mine = jnp.concatenate([r[...] for r in cols], axis=1)
    total = lax.dot_general(mine, cot_a[...], dims, preferred_element_type=F32)
    total += lax.dot_general(theirs[0], cot_b[...], dims, preferred_element_type=F32)
    top = jnp.full((TAIL, out.shape[-1]), jnp.maximum(jnp.max(jnp.abs(total)), 1e-30), F32)
    power = jnp.clip(jnp.ceil((jnp.log2(top) - 8.5) * 0.25), -14.0, 14.0)
    down = fourth(jnp.exp2(-power[:1]))
    row = lax.broadcasted_iota(jnp.int32, power.shape, 0)
    tail = jnp.exp2(jnp.where(row < TAIL // 2, power, -power))
    for k in range(4):
        out[k * BLOCK : k * BLOCK + DATA, :] = total[k * DATA : (k + 1) * DATA] * down
        out[k * BLOCK + DATA : (k + 1) * BLOCK, :] = tail


def grad_terms(chunks, tokens, cot, others, other_cot):
    rows, width = cot.shape
    count = len(chunks)
    whole = pl.BlockSpec((rows, width), lambda i, ids: (0, 0))
    call = pl.pallas_call(
        term_kernel,
        grid_spec=pltpu.PrefetchScalarGridSpec(
            num_scalar_prefetch=1,
            grid=(count,),
            in_specs=column_specs(rows) + [pl.BlockSpec((1, rows, 512), lambda i, ids: (i, 0, 0)), whole, whole],
            out_specs=pl.BlockSpec((4 * BLOCK, width), lambda i, ids: (i, 0)),
        ),
        out_shape=jax.ShapeDtypeStruct((4 * BLOCK * count, width), F32),
        compiler_params=pltpu.CompilerParams(vmem_limit_bytes=28 << 20),
        cost_estimate=pl.CostEstimate(
            flops=4 * rows * 512 * width * count, bytes_accessed=(2 + 3 * count) << 20, transcendentals=0
        ),
    )
    terms = call(jnp.concatenate(chunks).astype(jnp.int32), *[tokens] * 4, others, cot, other_cot)
    return [tall(terms[4 * BLOCK * k : 4 * BLOCK * (k + 1)]) for k in range(count)]


def sum_grad(tokens, cot, factor):
    z, x, y, c = (lax.axis_index(a) for a in FSDP)
    sign = 1 - 2 * c
    other_cot = lax.ppermute(cot, "c", SWAP)
    half = lambda v: v.astype(jnp.float16)
    steps = jnp.arange(4)
    up = (z + 4 - steps) % NZ
    down = jnp.where(steps == 0, z, z + 4 + steps) % NZ
    mine, theirs = jnp.where(c == 0, up, down), jnp.where(c == 0, down, up)
    near, far = (x + sign) % NX, (x + 2) % NX
    away = (x - sign) % NX
    first = pick_columns([theirs * NX + far], tokens)
    rest = pick_columns([mine * NX + away, theirs * NX + away, theirs * NX + x], tokens)
    first = lax.ppermute(first, "c", SWAP)
    rest = lax.ppermute(rest, "c", SWAP)
    (far_term,) = grad_terms([mine * NX + far], tokens, cot, first, other_cot)
    from_far = lax.ppermute(half(far_term), ("x", "c"), X_STEP)
    cross, near_term, own_term = grad_terms(
        [theirs * NX + near, mine * NX + near, mine * NX + x], tokens, cot, rest, other_cot
    )
    cross = half(cross)
    from_far, _ = lax.optimization_barrier((from_far, cross))
    cross = lax.ppermute(cross, ("x", "c"), X_STEP)
    cross = lax.ppermute(cross, "c", SWAP)
    direct = lax.ppermute(half(combine(near_term, from_far)), ("x", "c"), X_STEP)
    total = combine(own_term, cross, direct)
    straight = lax.ppermute(half(total[0:1]), ("z", "c"), Z_FAR)
    came = half(total[1:2])
    for k in range(1, 4):
        came = lax.ppermute(came, ("z", "c"), Z_STEP)
        if k < 3:
            came = half(combine(total[k + 1 : k + 2], came))
    plain = lambda v: v[0, :DATA].astype(F32) * fourth(scale_rows(v)[0][0])
    came = (plain(came) + jnp.where(c == 0, plain(straight), plain(total[0:1]))).reshape(2, 2, 32, -1)
    pick = lambda v, i, dim: lax.dynamic_index_in_dim(v, i, dim, keepdims=False)
    rows = pick(came, c, 1) + lax.ppermute(pick(came, 1 - c, 1), "c", SWAP)
    return (pick(rows, y, 0) + lax.ppermute(pick(rows, 1 - y, 0), "y", SWAP)) * factor


def token_kernel(where, *refs, count, halves):
    cot, blocks, out = refs[0], refs[1 : 1 + count], refs[-1]
    x = where[4]

    def one(block, base):
        got = lax.dot_general(
            cot[...], block[...], (((1,), (1,)), ((), ())), preferred_element_type=F32
        ).astype(out.dtype)
        for k in range(block.shape[0] // 128):
            col = lax.rem(x + base + k, NX)
            out[:, pl.ds(pl.multiple_of(col * 128, 128), 128)] = got[:, k * 128 : (k + 1) * 128]

    if halves:
        for k in range(count):
            one(blocks[k], where[5 + k])
    else:
        for k in range(count):
            pl.when(pl.program_id(0) == k)(functools.partial(one, blocks[k], 0))


def token_part(where, cot, blocks, done, halves=False):
    rows, width = cot.shape
    count = len(blocks)
    full = lambda s: pl.BlockSpec(s, lambda i, w: (0, 0))
    extra = [] if done is None else [done]
    size = sum(b.shape[0] for b in blocks)
    where = jnp.stack([jnp.asarray(v, jnp.int32) for v in where])
    return pl.pallas_call(
        functools.partial(token_kernel, count=count, halves=halves),
        grid_spec=pltpu.PrefetchScalarGridSpec(
            num_scalar_prefetch=1,
            grid=(1 if halves else count,),
            in_specs=[full((rows, width))]
            + [full(b.shape) for b in blocks]
            + [pl.BlockSpec(memory_space=pl.ANY)] * len(extra),
            out_specs=pl.BlockSpec((rows, 512), lambda i, w: (0, w[i])),
        ),
        out_shape=jax.ShapeDtypeStruct((rows, 4096), jnp.bfloat16),
        input_output_aliases={2 + count: 0} if extra else {},
        compiler_params=pltpu.CompilerParams(vmem_limit_bytes=20 << 20),
        cost_estimate=pl.CostEstimate(flops=2 * rows * size * width, bytes_accessed=4 << 20, transcendentals=0),
    )(where, cot, *blocks, *extra)


def token_grads(cot, weight):
    z, x, y, c = (lax.axis_index(a) for a in FSDP)
    sign = 1 - 2 * c
    ring = lambda step: [(i, (i + step) % NX) for i in range(NX)]
    other = lax.ppermute(weight, "y", SWAP)
    pair = jnp.where(y == 0, jnp.stack([weight, other]), jnp.stack([other, weight]))
    others = [lax.ppermute(pair, "x", ring(NX - k)) for k in (1, 2, 3)]
    mine = jnp.stack([pair, *others])
    theirs = lax.ppermute(mine, "c", SWAP)
    block = jnp.where(c == 0, jnp.stack([mine, theirs], 2), jnp.stack([theirs, mine], 2)).reshape(512, -1)
    near, swapped = [], []
    own = block
    for _ in range(1, 4):
        block = lax.ppermute(block, ("z", "c"), Z_STEP)
        near.append(block)
        swapped.append(lax.ppermute(block, "c", SWAP))
    block = lax.ppermute(lax.dynamic_slice_in_dim(block, 256 * c, 256, 0), ("z", "c"), Z_STEP)
    other = lax.ppermute(block, "c", SWAP)
    at = lambda k: (z + k * sign) % NZ
    grad = token_part((z, at(-1), at(1), 0, x), cot, [own, near[0], swapped[0]], None)
    grad = token_part((at(-2), at(2), 0, 0, x), cot, [near[1], swapped[1]], grad)
    grad = token_part((at(-3), at(3), 0, 0, x), cot, [near[2], swapped[2]], grad)
    return token_part((at(4), 0, 0, 0, x, 2 * c, 2 - 2 * c), cot, [block, other], grad, halves=True)


def step(tokens, value_cot, value_weight, global_params, local_params, momentum):
    mine = local_params[0]
    totals = mine + lax.ppermute(mine, "rep", SWAP)
    factor = 1.0 / jnp.sqrt(jnp.float32(tokens.shape[0] * lax.axis_size(FSDP)))
    token_grad = token_grads(value_cot, value_weight[0])
    value_grad = sum_grad(tokens, value_cot, factor)[None]
    pseudo = global_params - totals / lax.axis_size("rep")
    new_moment = 0.9 * momentum + pseudo
    new_global = global_params - 0.7 * (pseudo + 0.9 * new_moment)
    return (token_grad, value_grad, new_global, new_moment)


def solution(mesh):
    split = Mesh(mesh.devices.reshape(mesh.shape["rep"], NZ, NX, 2, 2), REP_FSDP)
    return jax.shard_map(
        step,
        mesh=split,
        in_specs=(
            P(REP_FSDP, None),
            P(REP_FSDP, None),
            P("rep", FSDP, None),
            P(FSDP),
            P("rep", FSDP),
            P(FSDP),
        ),
        out_specs=(P(REP_FSDP, None), P("rep", FSDP, None), P(FSDP), P(FSDP)),
        check_vma=False,
    )
```

```python
import functools

import jax
import jax.numpy as jnp
from jax import lax
from jax.experimental import pallas as pl
from jax.experimental.pallas import tpu as pltpu
from jax.sharding import Mesh
from jax.sharding import PartitionSpec as P


FSDP = ("z", "x", "y", "c")
REP_FSDP = ("rep", "z", "x", "y", "c")
NZ, NX = 8, 4
SWAP = [(0, 1), (1, 0)]
Z_STEP = [(2 * i + c, 2 * ((i + 1 - 2 * c) % NZ) + c) for i in range(NZ) for c in range(2)]
Z_FAR = [(2 * i, 2 * ((i + 4) % NZ)) for i in range(NZ)]
X_STEP = [(2 * i + c, 2 * ((i + 1 - 2 * c) % NX) + c) for i in range(NX) for c in range(2)]
F32 = jnp.float32
DATA, TAIL = 128, 8
BLOCK = DATA + TAIL


def tall(value):
    return value.reshape(-1, BLOCK, value.shape[-1])


def with_tails(body, up, down):
    row = lax.broadcasted_iota(jnp.int32, body.shape, 1)
    return jnp.where(row < DATA, body, jnp.where(row < DATA + TAIL // 2, up, down))


def scale_rows(value):
    low = DATA + TAIL // 2
    return value[0:1, DATA : DATA + 1].astype(F32), value[0:1, low : low + 1].astype(F32)


def fourth(v):
    return (v * v) * (v * v)


def combine(*parts):
    ups, downs = zip(*[scale_rows(p) for p in parts])
    up = functools.reduce(jnp.maximum, ups)
    down = functools.reduce(jnp.minimum, downs)
    body = sum(p.astype(F32) * fourth(u * down) for p, u in zip(parts, ups))
    return with_tails(body, up, down)


def chunk_copies(ids, tokens, place, sems, group):
    return [
        pltpu.make_async_copy(
            tokens.at[:, pl.ds(pl.multiple_of(ids[4 * group + k] * DATA, DATA), DATA)],
            place.at[group, :, pl.ds(k * DATA, DATA)],
            sems.at[4 * group + k],
        )
        for k in range(4)
    ]


def pick_kernel(ids, tokens, out, sems):
    copies = [copy for group in range(out.shape[0]) for copy in chunk_copies(ids, tokens, out, sems, group)]
    for copy in copies:
        copy.start()
    for copy in copies:
        copy.wait()


def pick_columns(chunks, tokens):
    rows = tokens.shape[0]
    count = len(chunks)
    return pl.pallas_call(
        pick_kernel,
        grid_spec=pltpu.PrefetchScalarGridSpec(
            num_scalar_prefetch=1,
            grid=(1,),
            in_specs=[pl.BlockSpec(memory_space=pltpu.HBM)],
            out_specs=pl.BlockSpec((count, rows, 512), lambda i, ids: (0, 0, 0)),
            scratch_shapes=[pltpu.SemaphoreType.DMA((4 * count,))],
        ),
        out_shape=jax.ShapeDtypeStruct((count, rows, 512), tokens.dtype),
        compiler_params=pltpu.CompilerParams(vmem_limit_bytes=16 << 20),
        cost_estimate=pl.CostEstimate(flops=rows * 512 * count, bytes_accessed=count << 20, transcendentals=0),
    )(jnp.concatenate(chunks).astype(jnp.int32), tokens)


def term_kernel(ids, tokens, theirs, cot_a, cot_b, out, cols, sems, *, count):
    step = pl.program_id(0)

    @pl.when(step == 0)
    def _():
        for group in range(count):
            for copy in chunk_copies(ids, tokens, cols, sems, group):
                copy.start()

    for group in range(count):

        @pl.when(step == group)
        def _():
            for copy in chunk_copies(ids, tokens, cols, sems, group):
                copy.wait()

    dims = (((0,), (0,)), ((), ()))
    total = lax.dot_general(cols[step], cot_a[...], dims, preferred_element_type=F32)
    total += lax.dot_general(theirs[0], cot_b[...], dims, preferred_element_type=F32)
    top = jnp.full((TAIL, out.shape[-1]), jnp.maximum(jnp.max(jnp.abs(total)), 1e-30), F32)
    power = jnp.clip(jnp.ceil((jnp.log2(top) - 8.5) * 0.25), -14.0, 14.0)
    down = fourth(jnp.exp2(-power[:1]))
    row = lax.broadcasted_iota(jnp.int32, power.shape, 0)
    tail = jnp.exp2(jnp.where(row < TAIL // 2, power, -power))
    for k in range(4):
        out[k * BLOCK : k * BLOCK + DATA, :] = total[k * DATA : (k + 1) * DATA] * down
        out[k * BLOCK + DATA : (k + 1) * BLOCK, :] = tail


def grad_terms(chunks, tokens, cot, others, other_cot):
    rows, width = cot.shape
    count = len(chunks)
    whole = pl.BlockSpec((rows, width), lambda i, ids: (0, 0))
    call = pl.pallas_call(
        functools.partial(term_kernel, count=count),
        grid_spec=pltpu.PrefetchScalarGridSpec(
            num_scalar_prefetch=1,
            grid=(count,),
            in_specs=[
                pl.BlockSpec(memory_space=pltpu.HBM),
                pl.BlockSpec((1, rows, 512), lambda i, ids: (i, 0, 0)),
                whole,
                whole,
            ],
            out_specs=pl.BlockSpec((4 * BLOCK, width), lambda i, ids: (i, 0)),
            scratch_shapes=[
                pltpu.VMEM((count, rows, 512), tokens.dtype),
                pltpu.SemaphoreType.DMA((4 * count,)),
            ],
        ),
        out_shape=jax.ShapeDtypeStruct((4 * BLOCK * count, width), F32),
        compiler_params=pltpu.CompilerParams(vmem_limit_bytes=28 << 20),
        cost_estimate=pl.CostEstimate(
            flops=4 * rows * 512 * width * count, bytes_accessed=(2 + 3 * count) << 20, transcendentals=0
        ),
    )
    terms = call(jnp.concatenate(chunks).astype(jnp.int32), tokens, others, cot, other_cot)
    return [tall(terms[4 * BLOCK * k : 4 * BLOCK * (k + 1)]) for k in range(count)]


def sum_grad(tokens, cot, factor):
    z, x, y, c = (lax.axis_index(a) for a in FSDP)
    sign = 1 - 2 * c
    other_cot = lax.ppermute(cot, "c", SWAP)
    half = lambda v: v.astype(jnp.float16)
    steps = jnp.arange(4)
    up = (z + 4 - steps) % NZ
    down = jnp.where(steps == 0, z, z + 4 + steps) % NZ
    mine, theirs = jnp.where(c == 0, up, down), jnp.where(c == 0, down, up)
    near, far = (x + sign) % NX, (x + 2) % NX
    away = (x - sign) % NX
    first = pick_columns([theirs * NX + far], tokens)
    rest = pick_columns([mine * NX + away, theirs * NX + away, theirs * NX + x], tokens)
    first = lax.ppermute(first, "c", SWAP)
    rest = lax.ppermute(rest, "c", SWAP)
    (far_term,) = grad_terms([mine * NX + far], tokens, cot, first, other_cot)
    from_far = lax.ppermute(half(far_term), ("x", "c"), X_STEP)
    cross, near_term, own_term = grad_terms(
        [theirs * NX + near, mine * NX + near, mine * NX + x], tokens, cot, rest, other_cot
    )
    cross = half(cross)
    from_far, _ = lax.optimization_barrier((from_far, cross))
    cross = lax.ppermute(cross, ("x", "c"), X_STEP)
    cross = lax.ppermute(cross, "c", SWAP)
    direct = lax.ppermute(half(combine(near_term, from_far)), ("x", "c"), X_STEP)
    held = lambda k: [v[k : k + 1] for v in (own_term, cross, direct)]
    came = half(combine(*held(1)))
    first = came
    for k in range(1, 4):
        came = lax.ppermute(came, ("z", "c"), Z_STEP)
        if k < 3:
            came = half(combine(*held(k + 1), came))
    rest, _ = lax.optimization_barrier((held(0), first))
    last = combine(*rest)
    straight = lax.ppermute(half(last), ("z", "c"), Z_FAR)
    value = lambda v: v.astype(F32) * fourth(scale_rows(v)[0])
    came = value(came) + jnp.where(c == 0, value(straight), value(last))
    came = came[0, :DATA].reshape(2, 2, 32, -1)
    pick = lambda v, i, dim: lax.dynamic_index_in_dim(v, i, dim, keepdims=False)
    rows = pick(came, c, 1) + lax.ppermute(pick(came, 1 - c, 1), "c", SWAP)
    return (pick(rows, y, 0) + lax.ppermute(pick(rows, 1 - y, 0), "y", SWAP)) * factor


def token_kernel(where, *refs, count, halves):
    cot, blocks, out = refs[0], refs[1 : 1 + count], refs[-1]
    x = where[4]

    def one(block, base):
        got = lax.dot_general(
            cot[...], block[...], (((1,), (1,)), ((), ())), preferred_element_type=F32
        ).astype(out.dtype)
        for k in range(block.shape[0] // 128):
            col = lax.rem(x + base + k, NX)
            out[:, pl.ds(pl.multiple_of(col * 128, 128), 128)] = got[:, k * 128 : (k + 1) * 128]

    if halves:
        for k in range(count):
            one(blocks[k], where[5 + k])
    else:
        for k in range(count):
            pl.when(pl.program_id(0) == k)(functools.partial(one, blocks[k], 0))


def token_part(where, cot, blocks, done, halves=False):
    rows, width = cot.shape
    count = len(blocks)
    full = lambda s: pl.BlockSpec(s, lambda i, w: (0, 0))
    extra = [] if done is None else [done]
    size = sum(b.shape[0] for b in blocks)
    where = jnp.stack([jnp.asarray(v, jnp.int32) for v in where])
    return pl.pallas_call(
        functools.partial(token_kernel, count=count, halves=halves),
        grid_spec=pltpu.PrefetchScalarGridSpec(
            num_scalar_prefetch=1,
            grid=(1 if halves else count,),
            in_specs=[full((rows, width))]
            + [full(b.shape) for b in blocks]
            + [pl.BlockSpec(memory_space=pl.ANY)] * len(extra),
            out_specs=pl.BlockSpec((rows, 512), lambda i, w: (0, w[i])),
        ),
        out_shape=jax.ShapeDtypeStruct((rows, 4096), jnp.bfloat16),
        input_output_aliases={2 + count: 0} if extra else {},
        compiler_params=pltpu.CompilerParams(vmem_limit_bytes=20 << 20),
        cost_estimate=pl.CostEstimate(flops=2 * rows * size * width, bytes_accessed=4 << 20, transcendentals=0),
    )(where, cot, *blocks, *extra)


def token_grads(cot, weight):
    z, x, y, c = (lax.axis_index(a) for a in FSDP)
    sign = 1 - 2 * c
    ring = lambda step: [(i, (i + step) % NX) for i in range(NX)]
    other = lax.ppermute(weight, "y", SWAP)
    pair = jnp.where(y == 0, jnp.stack([weight, other]), jnp.stack([other, weight]))
    others = [lax.ppermute(pair, "x", ring(NX - k)) for k in (1, 2, 3)]
    mine = jnp.stack([pair, *others])
    theirs = lax.ppermute(mine, "c", SWAP)
    block = jnp.where(c == 0, jnp.stack([mine, theirs], 2), jnp.stack([theirs, mine], 2)).reshape(512, -1)
    near, swapped = [], []
    own = block
    for _ in range(1, 4):
        block = lax.ppermute(block, ("z", "c"), Z_STEP)
        near.append(block)
        swapped.append(lax.ppermute(block, "c", SWAP))
    block = lax.ppermute(lax.dynamic_slice_in_dim(block, 256 * c, 256, 0), ("z", "c"), Z_STEP)
    other = lax.ppermute(block, "c", SWAP)
    at = lambda k: (z + k * sign) % NZ
    grad = token_part((z, at(-1), at(1), 0, x), cot, [own, near[0], swapped[0]], None)
    grad = token_part((at(-2), at(2), 0, 0, x), cot, [near[1], swapped[1]], grad)
    grad = token_part((at(-3), at(3), 0, 0, x), cot, [near[2], swapped[2]], grad)
    return token_part((at(4), 0, 0, 0, x, 2 * c, 2 - 2 * c), cot, [block, other], grad, halves=True)


def step(tokens, value_cot, value_weight, global_params, local_params, momentum):
    mine = local_params[0]
    totals = mine + lax.ppermute(mine, "rep", SWAP)
    factor = 1.0 / jnp.sqrt(jnp.float32(tokens.shape[0] * lax.axis_size(FSDP)))
    token_grad = token_grads(value_cot, value_weight[0])
    value_grad = sum_grad(tokens, value_cot, factor)[None]
    pseudo = global_params - totals / lax.axis_size("rep")
    new_moment = 0.9 * momentum + pseudo
    new_global = global_params - 0.7 * (pseudo + 0.9 * new_moment)
    return (token_grad, value_grad, new_global, new_moment)


def solution(mesh):
    split = Mesh(mesh.devices.reshape(mesh.shape["rep"], NZ, NX, 2, 2), REP_FSDP)
    return jax.shard_map(
        step,
        mesh=split,
        in_specs=(
            P(REP_FSDP, None),
            P(REP_FSDP, None),
            P("rep", FSDP, None),
            P(FSDP),
            P("rep", FSDP),
            P(FSDP),
        ),
        out_specs=(P(REP_FSDP, None), P("rep", FSDP, None), P(FSDP), P(FSDP)),
        check_vma=False,
    )
```
